1024 devices in a mesh: pipe: 8 (over z), dp: 4 (over x_lo, core), expert: 32 (over y, x_hi).
Axes of the slice: x: 8 (x_hi: 4, x_lo: 2; x = x_hi * 2 + x_lo), y: 8, z: 8, core: 2. Of those that a mesh axis runs over, the one named last changes fastest.
Arguments:
- cotangent: bfloat16 [8, 8192, 7168], P('pipe', ('dp', 'expert')), may hold values from -6 to 6
- routes: int32 [8, 2, 8192, 8], P('pipe', None, ('dp', 'expert')), may hold values from 0 to 255, as said below
- gates: bfloat16 [8, 2, 8192, 8], P('pipe', None, ('dp', 'expert')), may hold values from 0.099609375 to 1
- gate_pre: bfloat16 [8, 2, 4, 32, 2, 4096], P('pipe', None, 'dp', None, None, 'expert'), may hold values from -6 to 6
- up_pre: bfloat16 [8, 2, 4, 32, 2, 4096], P('pipe', None, 'dp', None, None, 'expert'), may hold values from -6 to 6
- w_gate: bfloat16 [8, 7168, 4096], P('pipe', None, 'expert'), may hold values from -0.0625 to 0.0625
- w_up: bfloat16 [8, 7168, 4096], P('pipe', None, 'expert'), may hold values from -0.0625 to 0.0625
- w_down: bfloat16 [8, 4096, 7168], P('pipe', 'expert'), may hold values from -0.125 to 0.125
Outputs:
- down_grad: float32 [8, 4096, 7168], P('pipe', 'expert', 'dp')
The draws below stay inside these ranges and needn't reach their ends.
Inputs may be any that keep to these rules, and one draw needn't show every extreme that they name: `routes`: each token names 8 different experts. At one section and step the tokens of one device name each of the experts 0 to 1 at least once and at most 2 times; at every section and step, in some replica every device names one of them exactly 2 times.
All inputs are finite; a program needn't handle non-finite values.
Results may differ from the reference program's by a relative error of at most 0.0095.
Values may be sent and summed in bfloat16 or wider, within the bound.
No kernel may reach another device: no remote copies, remote signals or barrier semaphores. Data moves between devices by JAX's collectives and lax.ppermute only.
A program may use at most 64 MiB of HBM per device.

```python
import math
import jax
import jax.numpy as jnp
from jax import lax

D = 7168
FFE = 2048
EXPERTS = 256
TOPK = 8
EXP_FL = 2
STEPS = 2
TOK_DEV = 64
CAP = 2
TOKENS = 8192
N_PIPE = 8
N_DP = 4
N_EXPERT = 32


def draw_routes(key, part):
    keys = jax.random.split(key, 6)
    lead = (N_PIPE, STEPS, N_DP, N_EXPERT)
    counts = jax.random.randint(keys[0], lead + (EXP_FL,), 1, CAP + 1)
    full_rep = jax.random.randint(keys[1], (N_PIPE, STEPS, 1, 1, 1), 0, N_DP)
    full_exp = jax.random.randint(keys[2], (N_PIPE, STEPS, 1, 1, 1), 0, EXP_FL)
    rep_index = jnp.arange(N_DP).reshape(1, 1, N_DP, 1, 1)
    exp_index = jnp.arange(EXP_FL).reshape(1, 1, 1, 1, EXP_FL)
    counts = jnp.where((rep_index == full_rep) & (exp_index == full_exp), CAP, counts)
    scores = jax.random.randint(keys[3], lead + (EXP_FL, TOK_DEV), 0, 1 << 20) * TOK_DEV + jnp.arange(TOK_DEV)
    ranking = jnp.argsort(jnp.argsort(scores, axis=-1), axis=-1)
    chosen = ranking < counts[..., None]
    chosen = jnp.moveaxis(chosen, -2, -1)
    others = jax.random.randint(keys[4], lead + (TOK_DEV, EXPERTS - EXP_FL), 0, 1 << 16) * EXPERTS + jnp.arange(EXPERTS - EXP_FL)
    picked = lax.top_k(others, TOPK)[1] + EXP_FL
    head = jnp.where(chosen, jnp.arange(EXP_FL), picked[..., :EXP_FL])
    named = jnp.concatenate([head, picked[..., EXP_FL:]], axis=-1)
    order = jax.random.randint(keys[5], lead + (TOK_DEV, TOPK), 0, 1 << 20) * TOPK + jnp.arange(TOPK)
    shuffle = jnp.argsort(order, axis=-1)
    named = jnp.take_along_axis(named, shuffle, axis=-1)
    return named.reshape(N_PIPE, STEPS, N_DP * N_EXPERT * TOK_DEV, TOPK).astype(jnp.int32)


def steps_of(own_key, shape, cuts, least, largest):
    def one(axis_at, shards_of):
        heights = jax.random.uniform(jax.random.fold_in(jax.random.fold_in(own_key, 6), axis_at), (shards_of,), jnp.float32, least / len(cuts), largest / len(cuts))
        return jnp.repeat(jnp.exp(heights), shape[axis_at] // shards_of).reshape((-1,) + (1,) * (len(shape) - axis_at - 1))

    level = one(*cuts[0])
    for cut in cuts[1:]:
        level = level * one(*cut)
    return level


def scatter_about(rng, dims, scale, reach, pieces=(), held_as=jnp.bfloat16):
    entries = scale * jax.random.normal(rng, dims, jnp.float32)
    if pieces:
        entries = entries * steps_of(rng, dims, pieces, -0.22, 0.18)
    return jnp.clip(entries, -reach, reach).astype(held_as)


def setup_inputs(seed: int = 0) -> dict:
    arg_keys = jax.random.split(jax.random.key(seed), 9)
    cotangent = scatter_about(arg_keys[0], (N_PIPE, TOKENS, D), 1.0, 6.0, ((0, 8), (1, 128)))
    routes = draw_routes(jax.random.fold_in(arg_keys[8], 71), 0)
    gates = jnp.clip(jnp.exp(math.log(1.0) - 2.306499 * jax.random.uniform(arg_keys[2], (N_PIPE, STEPS, TOKENS, TOPK), jnp.float32) ** steps_of(arg_keys[2], (N_PIPE, STEPS, TOKENS, TOPK), ((0, 8), (2, 128)), -0.2, 0.2)), 0.099609375, 1.0).astype(jnp.bfloat16)
    gate_pre = scatter_about(arg_keys[3], (N_PIPE, STEPS, N_DP, N_EXPERT, CAP, EXP_FL * FFE), 1.0, 6.0, ((0, 8), (2, 4), (5, 32)))
    up_pre = scatter_about(arg_keys[4], (N_PIPE, STEPS, N_DP, N_EXPERT, CAP, EXP_FL * FFE), 1.0, 6.0, ((0, 8), (2, 4), (5, 32)))
    w_gate = scatter_about(arg_keys[5], (N_PIPE, D, EXP_FL * FFE), D ** -0.5, 0.0625, ((0, 8), (2, 32)))
    w_up = scatter_about(arg_keys[6], (N_PIPE, D, EXP_FL * FFE), D ** -0.5, 0.0625, ((0, 8), (2, 32)))
    w_down = scatter_about(arg_keys[7], (N_PIPE, EXP_FL * FFE, D), FFE ** -0.5, 0.125, ((0, 8), (1, 32)))
    return {"cotangent": cotangent, "routes": routes, "gates": gates, "gate_pre": gate_pre, "up_pre": up_pre, "w_gate": w_gate, "w_up": w_up, "w_down": w_down}


def slot_tables(ids, weights):
    match = (ids[..., None] == jnp.arange(EXP_FL, dtype=jnp.int32)).astype(jnp.float32)
    hit = jnp.sum(match, axis=2)
    gate_sum = jnp.sum(match * weights.astype(jnp.float32)[..., None, None].reshape(match.shape[:3] + (1,)), axis=2)
    rank = jnp.cumsum(hit, axis=1) - 1.0
    slots = jnp.arange(CAP, dtype=jnp.float32)
    select = hit[..., None] * (rank[..., None] == slots).astype(jnp.float32)
    select = jnp.transpose(select, (0, 2, 3, 1))
    slot_gate = jnp.einsum('bect,bte->bec', select, gate_sum)
    return select, slot_gate


def reference(cotangent, routes, gates, gate_pre, up_pre, w_gate, w_up, w_down):
    blocks = N_DP * N_EXPERT
    split = N_EXPERT // EXP_FL
    hidden = FFE // split
    state = cotangent
    total = jnp.zeros((N_PIPE, EXP_FL * FFE, D), jnp.float32)
    for step in range(STEPS):
        produced = []
        for section in range(N_PIPE):
            grad_in = state[section].reshape(blocks, TOK_DEV, D)
            ids = routes[section, step].reshape(blocks, TOK_DEV, TOPK)
            weights = gates[section, step].reshape(blocks, TOK_DEV, TOPK)
            select, slot_gate = slot_tables(ids, weights)
            rows = jnp.einsum('bect,btd->becd', select, grad_in.astype(jnp.float32)).astype(jnp.bfloat16)
            grad_out = grad_in.astype(jnp.float32)
            pre_gate_all = gate_pre[section, step].reshape(blocks * CAP, EXP_FL * FFE)
            pre_up_all = up_pre[section, step].reshape(blocks * CAP, EXP_FL * FFE)
            for expert in range(EXP_FL):
                lower = expert * FFE
                flat_rows = rows[:, expert].reshape(blocks * CAP, D)
                gate_col = slot_gate[:, expert].reshape(blocks * CAP, 1)
                pre_u = pre_gate_all[:, lower:lower + FFE].astype(jnp.float32)
                pre_v = pre_up_all[:, lower:lower + FFE].astype(jnp.float32)
                down_rows = w_down[section, lower:lower + FFE]
                grad_act = gate_col * jnp.dot(flat_rows, down_rows.T, preferred_element_type=jnp.float32)
                sig = jax.nn.sigmoid(pre_u)
                act = pre_u * sig
                dsilu = sig * (1.0 + pre_u * (1.0 - sig))
                d_gate = (grad_act * pre_v * dsilu).astype(jnp.bfloat16)
                d_up = (grad_act * act).astype(jnp.bfloat16)
                scaled = (gate_col * act * pre_v).astype(jnp.bfloat16)
                term = jnp.dot(scaled.T, flat_rows, preferred_element_type=jnp.float32)
                total = total.at[section, lower:lower + FFE].add(term)
                if step + 1 < STEPS:
                    gate_cols = w_gate[section][:, lower:lower + FFE].reshape(D, split, hidden).astype(jnp.float32)
                    up_cols = w_up[section][:, lower:lower + FFE].reshape(D, split, hidden).astype(jnp.float32)
                    dg = d_gate.reshape(blocks * CAP, split, hidden).astype(jnp.float32)
                    du = d_up.reshape(blocks * CAP, split, hidden).astype(jnp.float32)
                    parts = jnp.einsum('rjh,djh->jrd', dg, gate_cols) + jnp.einsum('rjh,djh->jrd', du, up_cols)
                    parts = parts.astype(jnp.bfloat16).astype(jnp.float32)
                    summed = jnp.sum(parts, axis=0).reshape(blocks, CAP, D)
                    grad_out = grad_out + jnp.einsum('bct,bcd->btd', select[:, expert], summed)
            produced.append(grad_out.astype(jnp.bfloat16).reshape(TOKENS, D))
        if step + 1 < STEPS:
            state = jnp.stack(produced[1:] + [jnp.zeros((TOKENS, D), jnp.bfloat16)])
    return total
```

```python
import jax
import jax.numpy as jnp
from jax import lax
from jax.experimental import pallas as pl
from jax.experimental.pallas import tpu as pltpu
from jax.sharding import PartitionSpec as P

EXP_FL = 2
N_DP = 4
F32 = jnp.float32
BF16 = jnp.bfloat16
VMEM = pl.BlockSpec(memory_space=pltpu.VMEM)
SMEM = pl.BlockSpec(memory_space=pltpu.SMEM)


def mm(a, b, ca, cb, precision=None):
    return lax.dot_general(
        a, b, (((ca,), (cb,)), ((), ())), preferred_element_type=F32, precision=precision
    )


def iota(shape, dim):
    return lax.broadcasted_iota(jnp.int32, shape, dim)


def slice_of(row):
    return (row >> 1) & 3


def select_kernel(ids_ref, gates_ref, cot_ref, pay_ref, sel_ref, up_ref):
    n, _, width = pay_ref.shape
    tokens = cot_ref.shape[0]
    row = iota((16, tokens), 0)
    slot = (row & 1).astype(F32)
    before = (iota((tokens, tokens), 0) <= iota((tokens, tokens), 1)).astype(BF16)

    def tables(step):
        ids = ids_ref[step]
        weights = gates_ref[step].astype(F32)
        hits, sums = [], []
        for e in range(EXP_FL):
            match = (ids == e).astype(F32)
            hits.append(jnp.sum(match, axis=0, keepdims=True))
            sums.append(jnp.sum(match * weights, axis=0, keepdims=True))
        hit = jnp.where(row < 8, hits[0], hits[1])
        gate = jnp.where(row < 8, sums[0], sums[1])
        rank = mm(hit.astype(BF16), before, 1, 0) - 1.0
        return hit * (rank == slot).astype(F32), gate

    sel0, gate0 = tables(0)
    sel1, gate1 = tables(1)
    sel_ref[...] = sel0.astype(BF16)
    up_ref[...] = (sel1 * gate1).astype(BF16)
    pick = sel0 * gate0
    rows = jnp.zeros((16, width), F32)
    for q in range(N_DP):
        left = jnp.where(slice_of(row) == q, pick, 0.0).astype(BF16)
        rows = rows + mm(left, cot_ref[:, q * width : (q + 1) * width], 1, 0)
    rows = rows.astype(BF16)
    for t in range(n):
        pay_ref[t] = rows[:8] if t < n // 2 else rows[8:]


def expert_kernel(
    me_ref, x_ref, u_ref, v_ref, wd_ref, wg_ref, wu_ref, ret_ref, x0_ref, x1_ref, x2_ref, x3_ref
):
    me = me_ref[0]
    rows, width = x_ref.shape
    slots = rows // N_DP
    hidden = wd_ref.shape[0]
    grad = jnp.zeros((rows, hidden), F32)
    part = slice_of(iota((rows, hidden), 0))
    for q in range(N_DP):
        term = mm(x_ref[...], wd_ref[:, q * width : (q + 1) * width], 1, 1)
        grad = jnp.where(part == q, term, grad)
    grad = grad.reshape(rows // 8, 8, hidden)
    grad = grad + pltpu.roll(grad, 4, 1)
    grad = grad + pltpu.roll(grad, 2, 1)
    grad = grad.reshape(rows, hidden)
    wide = iota((rows, slots), 0)
    spread = (iota((rows, slots), 1) == 2 * (wide >> 3) + (wide & 1)).astype(BF16)
    u = mm(spread, u_ref[0], 1, 0)
    v = mm(spread, v_ref[0], 1, 0)
    sig = jax.nn.sigmoid(u)
    d_gate = grad * v * sig * (1.0 + u * (1.0 - sig))
    d_up = grad * (u * sig)
    both = jnp.concatenate([d_gate, d_up], axis=1)
    part = slice_of(iota((rows, 2 * hidden), 0))
    lefts = [jnp.where(part == q, both, 0.0).astype(BF16) for q in range(N_DP)]
    tile = min(256, width)
    for n in range(width // tile):
        acc = jnp.zeros((rows, tile), F32)
        for q in range(N_DP):
            at = q * width + n * tile
            right = jnp.concatenate([wg_ref[at : at + tile], wu_ref[at : at + tile]], axis=1)
            acc = acc + mm(lefts[q], right, 1, 1)
        ret_ref[:, n * tile : (n + 1) * tile] = acc.astype(BF16)
    acts = []
    for step in range(2):
        u = u_ref[step].astype(F32)
        v = v_ref[step].astype(F32)
        acts.append((u * jax.nn.sigmoid(u) * v).astype(BF16))
    low = iota((slots, rows), 0)
    wide = iota((slots, rows), 1)
    mine = (low >> 1 == wide >> 3) & (low & 1 == wide & 1)
    for k, out_ref in enumerate((x0_ref, x1_ref, x2_ref, x3_ref)):
        pick = (mine & (slice_of(wide) == (me ^ k))).astype(BF16)
        out_ref[:, :width] = mm(pick, x_ref[...], 1, 0).astype(BF16)
        out_ref[:, width : width + hidden] = acts[0]
        out_ref[:, width + hidden :] = acts[1]


def combine_kernel(back_ref, up_ref, sel_ref, cot_ref, out_ref):
    n, _, width = back_ref.shape
    sums = [jnp.sum(back_ref[e * (n // 2) : (e + 1) * (n // 2)].astype(F32), axis=0) for e in range(EXP_FL)]
    back = jnp.concatenate(sums, axis=0)
    up = up_ref[...]
    meet = mm(up, sel_ref[...], 1, 1)
    meet = jnp.where(slice_of(iota((16, 16), 0)) == slice_of(iota((16, 16), 1)), meet, 0.0)
    out = mm(meet, back, 1, 0, lax.Precision.HIGHEST)
    row = slice_of(iota(up.shape, 0))
    for q in range(N_DP):
        left = jnp.where(row == q, up, jnp.zeros_like(up))
        out = out + mm(left, cot_ref[:, q * width : (q + 1) * width], 1, 0)
    out_ref[...] = out.astype(BF16)


def first_kernel(x0_ref, x1_ref, x2_ref, x3_ref, out_ref):
    hidden, width = out_ref.shape
    acc = jnp.zeros((hidden, width), F32)
    for ref in (x0_ref, x1_ref, x2_ref, x3_ref):
        acc = acc + mm(ref[:, width : width + hidden], ref[:, :width], 0, 0)
    out_ref[...] = acc


def second_kernel(me_ref, acc_ref, y_ref, x0_ref, x1_ref, x2_ref, x3_ref, out_ref):
    me = me_ref[0]
    hidden, width = out_ref.shape
    slots = x0_ref.shape[0]
    acc = acc_ref[...]
    for k, ref in enumerate((x0_ref, x1_ref, x2_ref, x3_ref)):
        at = pl.multiple_of((me ^ k) * slots, slots)
        acc = acc + mm(ref[:, width + hidden :], y_ref[pl.ds(at, slots), :], 0, 0)
    out_ref[...] = acc


def call(kernel, outs, specs, flops, moved, name):
    return pl.pallas_call(
        kernel,
        out_shape=outs,
        in_specs=specs,
        out_specs=jax.tree.map(lambda _: VMEM, outs),
        cost_estimate=pl.CostEstimate(flops=flops, bytes_accessed=moved, transcendentals=0),
        name=name,
    )


def like(shape, dtype=BF16):
    return jax.ShapeDtypeStruct(shape, dtype)


def body(cotangent, routes, gates, gate_pre, up_pre, w_gate, w_up, w_down):
    n = lax.axis_size("expert")
    pipe = lax.axis_size("pipe")
    cot = cotangent[0]
    tokens, full = cot.shape
    width = full // N_DP
    hidden = gate_pre.shape[5]
    slots = 2 * n
    me = lax.axis_index("dp").astype(jnp.int32).reshape(1)
    ids = jnp.swapaxes(routes[0], 1, 2)
    weights = jnp.swapaxes(gates[0], 1, 2)
    pay, sel0, up = call(
        select_kernel,
        (like((n, 8, width)), like((16, tokens)), like((16, tokens))),
        [VMEM] * 3,
        10**8,
        2 * 10**6,
        "select",
    )(ids, weights, cot)
    up = lax.ppermute(up, "pipe", [(i, i + 1) for i in range(pipe - 1)])
    got = lax.all_to_all(pay, "expert", 0, 0, tiled=True)
    u = gate_pre[0].reshape(2, slots, hidden)
    v = up_pre[0].reshape(2, slots, hidden)
    piece = like((slots, width + 2 * hidden))
    ret, x0, x1, x2, x3 = call(
        expert_kernel,
        (like((8 * n, width)), piece, piece, piece, piece),
        [SMEM] + [VMEM] * 6,
        2 * 10**9,
        8 * 10**6,
        "expert",
    )(me, got.reshape(8 * n, width), u, v, w_down[0], w_gate[0], w_up[0])
    back = lax.all_to_all(ret.reshape(n, 8, width), "expert", 0, 0, tiled=True)
    rows = call(combine_kernel, like((16, width)), [VMEM] * 4, 10**8, 2 * 10**6, "combine")(
        back, up, sel0, cot
    )
    rows = lax.ppermute(rows, "pipe", [(i, i - 1) for i in range(1, pipe)])
    x1 = lax.ppermute(x1, "dp", [(i, i ^ 1) for i in range(N_DP)])
    x2 = lax.ppermute(x2, "dp", [(i, i ^ 2) for i in range(N_DP)])
    x3 = lax.ppermute(x3, "dp", [(i, i ^ 3) for i in range(N_DP)])
    rows = rows.reshape(EXP_FL, N_DP, 1, 2, width).swapaxes(0, 1)
    rows = jnp.broadcast_to(rows, (N_DP, EXP_FL, n // EXP_FL, 2, width))
    got = lax.all_to_all(rows.reshape(N_DP * n, 2, width), ("dp", "expert"), 0, 0, tiled=True)
    acc = call(first_kernel, like((hidden, width), F32), [VMEM] * 4, 10**8, 2 * 10**6, "first")(
        x0, x1, x2, x3
    )
    out = call(
        second_kernel, like((hidden, width), F32), [SMEM] + [VMEM] * 6, 10**8, 2 * 10**6, "second"
    )(me, acc, got.reshape(N_DP * slots, width), x0, x1, x2, x3)
    return out[None]


def solution(mesh):
    in_specs = (
        P("pipe", ("dp", "expert"), None),
        P("pipe", None, ("dp", "expert"), None),
        P("pipe", None, ("dp", "expert"), None),
        P("pipe", None, "dp", None, None, "expert"),
        P("pipe", None, "dp", None, None, "expert"),
        P("pipe", None, "expert"),
        P("pipe", None, "expert"),
        P("pipe", "expert", None),
    )
    out_specs = P("pipe", "expert", "dp")
    return jax.shard_map(body, mesh=mesh, in_specs=in_specs, out_specs=out_specs, check_vma=False)
```

```python
import jax
import jax.numpy as jnp
from jax import lax
from jax.experimental import pallas as pl
from jax.experimental.pallas import tpu as pltpu
from jax.sharding import PartitionSpec as P

EXP_FL = 2
N_DP = 4
F32 = jnp.float32
BF16 = jnp.bfloat16
VMEM = pl.BlockSpec(memory_space=pltpu.VMEM)
SMEM = pl.BlockSpec(memory_space=pltpu.SMEM)


def mm(a, b, ca, cb, precision=None):
    return lax.dot_general(
        a, b, (((ca,), (cb,)), ((), ())), preferred_element_type=F32, precision=precision
    )


def iota(shape, dim):
    return lax.broadcasted_iota(jnp.int32, shape, dim)


def slice_of(row):
    return (row >> 1) & 3


def select_kernel(ids_ref, gates_ref, cot_hbm, pay_ref, sel_ref, up_ref, cot_ref, sem):
    n, _, width = pay_ref.shape
    tokens = cot_ref.shape[0]
    copy = pltpu.make_async_copy(cot_hbm, cot_ref, sem)
    copy.start()
    row = iota((16, tokens), 0)
    slot = (row & 1).astype(F32)
    before = (iota((tokens, tokens), 0) <= iota((tokens, tokens), 1)).astype(BF16)

    def tables(step):
        ids = ids_ref[step]
        weights = gates_ref[step].astype(F32)
        hits, sums = [], []
        for e in range(EXP_FL):
            match = (ids == e).astype(F32)
            hits.append(jnp.sum(match, axis=0, keepdims=True))
            sums.append(jnp.sum(match * weights, axis=0, keepdims=True))
        hit = jnp.where(row < 8, hits[0], hits[1])
        gate = jnp.where(row < 8, sums[0], sums[1])
        rank = mm(hit.astype(BF16), before, 1, 0) - 1.0
        return hit * (rank == slot).astype(F32), gate

    sel0, gate0 = tables(0)
    sel1, gate1 = tables(1)
    sel_ref[...] = sel0.astype(BF16)
    up_ref[...] = (sel1 * gate1).astype(BF16)
    lefts = split(sel0 * gate0)
    copy.wait()
    rows = gathered(lefts, cot_ref, width).astype(BF16)
    for t in range(n):
        pay_ref[t] = rows[:8] if t < n // 2 else rows[8:]


def split(pick):
    row = slice_of(iota(pick.shape, 0))
    return [jnp.where(row == q, pick, 0.0).astype(BF16) for q in range(N_DP)]


def gathered(lefts, cot_ref, width):
    rows = mm(lefts[0], cot_ref[:, :width], 1, 0)
    for q in range(1, N_DP):
        rows = rows + mm(lefts[q], cot_ref[:, q * width : (q + 1) * width], 1, 0)
    return rows


def expert_kernel(
    me_ref,
    x_ref,
    u_ref,
    v_ref,
    wd_hbm,
    wg_hbm,
    wu_hbm,
    ret_ref,
    x0_ref,
    x1_ref,
    x2_ref,
    x3_ref,
    wd_ref,
    wg_ref,
    wu_ref,
    sems,
):
    copies = [
        pltpu.make_async_copy(src, dst, sems.at[k])
        for k, (src, dst) in enumerate(((wd_hbm, wd_ref), (wg_hbm, wg_ref), (wu_hbm, wu_ref)))
    ]
    for copy in copies:
        copy.start()
    me = me_ref[0]
    rows, width = x_ref.shape
    slots = rows // N_DP
    hidden = wd_ref.shape[0]
    acts = []
    for step in range(2):
        u = u_ref[step].astype(F32)
        v = v_ref[step].astype(F32)
        acts.append((u * jax.nn.sigmoid(u) * v).astype(BF16))
    low = iota((rows, rows), 0)
    wide = iota((rows, rows), 1)
    to = low // slots
    low = low - to * slots
    pick = (low >> 1 == wide >> 3) & (low & 1 == wide & 1) & (slice_of(wide) == (me ^ to))
    moved = mm(pick.astype(BF16), x_ref[...], 1, 0).astype(BF16)
    for k, out_ref in enumerate((x0_ref, x1_ref, x2_ref, x3_ref)):
        out_ref[:, :width] = moved[k * slots : (k + 1) * slots]
        out_ref[:, width : width + hidden] = acts[0]
        out_ref[:, width + hidden :] = acts[1]
    wide = iota((rows, slots), 0)
    spread = (iota((rows, slots), 1) == 2 * (wide >> 3) + (wide & 1)).astype(BF16)
    u = mm(spread, u_ref[0], 1, 0)
    v = mm(spread, v_ref[0], 1, 0)
    sig = jax.nn.sigmoid(u)
    for_gate = v * sig * (1.0 + u * (1.0 - sig))
    for_up = u * sig
    copies[0].wait()
    right = jnp.concatenate([wd_ref[:, q * width : (q + 1) * width] for q in range(N_DP)], axis=0)
    terms = mm(x_ref[...], right, 1, 1)
    part = slice_of(iota((rows, hidden), 0))
    grad = terms[:, :hidden]
    for q in range(1, N_DP):
        grad = jnp.where(part == q, terms[:, q * hidden : (q + 1) * hidden], grad)
    grad = grad.reshape(rows // 8, 8, hidden)
    grad = grad + pltpu.roll(grad, 4, 1)
    grad = grad + pltpu.roll(grad, 2, 1)
    grad = grad.reshape(rows, hidden)
    lefts = split(jnp.concatenate([grad * for_gate, grad * for_up], axis=1))
    copies[1].wait()
    copies[2].wait()
    tile = min(256, width)
    for n in range(width // tile):
        acc = None
        for q in range(N_DP):
            at = q * width + n * tile
            right = jnp.concatenate([wg_ref[at : at + tile], wu_ref[at : at + tile]], axis=1)
            term = mm(lefts[q], right, 1, 1)
            acc = term if acc is None else acc + term
        ret_ref[:, n * tile : (n + 1) * tile] = acc.astype(BF16)


def token_kernel(up_ref, sel_ref, cot_hbm, rows_ref, meet_ref, cot_ref, sem):
    copy = pltpu.make_async_copy(cot_hbm, cot_ref, sem)
    copy.start()
    up = up_ref[...]
    meet = mm(up, sel_ref[...], 1, 1)
    same = slice_of(iota((16, 16), 0)) == slice_of(iota((16, 16), 1))
    meet_ref[...] = jnp.where(same, meet, 0.0)
    copy.wait()
    rows_ref[...] = gathered(split(up.astype(F32)), cot_ref, rows_ref.shape[1])


def combine_kernel(back_ref, rows_ref, meet_ref, out_ref):
    n = back_ref.shape[0]
    half = n // EXP_FL
    sums = [jnp.sum(back_ref[e * half : (e + 1) * half].astype(F32), axis=0) for e in range(EXP_FL)]
    back = jnp.concatenate(sums, axis=0)
    out = rows_ref[...] + mm(meet_ref[...], back, 1, 0, lax.Precision.HIGHEST)
    out_ref[...] = out.astype(BF16)


def first_kernel(x0_ref, x1_ref, x2_ref, x3_ref, out_ref):
    hidden, width = out_ref.shape
    acc = None
    for ref in (x0_ref, x1_ref, x2_ref, x3_ref):
        term = mm(ref[:, width : width + hidden], ref[:, :width], 0, 0)
        acc = term if acc is None else acc + term
    out_ref[...] = acc


def second_kernel(me_ref, acc_ref, y_ref, x0_ref, x1_ref, x2_ref, x3_ref, out_ref):
    me = me_ref[0]
    hidden, width = out_ref.shape
    slots = x0_ref.shape[0]
    acc = acc_ref[...]
    for k, ref in enumerate((x0_ref, x1_ref, x2_ref, x3_ref)):
        at = pl.multiple_of((me ^ k) * slots, slots)
        acc = acc + mm(ref[:, width + hidden :], y_ref[pl.ds(at, slots), :], 0, 0)
    out_ref[...] = acc


def call(kernel, outs, flops, moved, ins, out_in_hbm=False, held=(), **kwargs):
    specs = [SMEM if x.dtype == jnp.int32 and x.ndim == 1 else VMEM for x in ins]
    specs[len(ins) - len(held) :] = [pl.BlockSpec(memory_space=pl.ANY)] * len(held)
    shapes = [like(*o) if out_in_hbm or not ON_CHIP else pltpu.VMEM(*o) for o in outs]
    return pl.pallas_call(
        kernel,
        out_shape=shapes,
        in_specs=specs,
        out_specs=[VMEM] * len(outs),
        cost_estimate=pl.CostEstimate(flops=flops, bytes_accessed=moved, transcendentals=0),
        compiler_params=pltpu.CompilerParams(vmem_limit_bytes=24 << 20),
        **kwargs,
    )(*ins)


def in_hbm(x):
    return pltpu.with_memory_space_constraint(x, pltpu.HBM) if ON_CHIP else x


def like(shape, dtype=BF16):
    return jax.ShapeDtypeStruct(shape, dtype)


ON_CHIP = True


def body(cotangent, routes, gates, gate_pre, up_pre, w_gate, w_up, w_down):
    n = lax.axis_size("expert")
    pipe = lax.axis_size("pipe")
    cot = cotangent[0]
    tokens, full = cot.shape
    width = full // N_DP
    hidden = gate_pre.shape[5]
    slots = 2 * n
    me = lax.axis_index("dp").astype(jnp.int32).reshape(1)
    ids = jnp.swapaxes(routes[0], 1, 2)
    weights = jnp.swapaxes(gates[0], 1, 2)
    pay, sel0, up = pl.pallas_call(
        select_kernel,
        out_shape=[(pltpu.VMEM if ON_CHIP else like)(s, BF16) for s in ((n, 8, width), (16, tokens), (16, tokens))],
        in_specs=[VMEM, VMEM, pl.BlockSpec(memory_space=pl.ANY)],
        out_specs=[VMEM] * 3,
        scratch_shapes=[pltpu.VMEM(cot.shape, BF16), pltpu.SemaphoreType.DMA(())],
        cost_estimate=pl.CostEstimate(flops=10**8, bytes_accessed=2 * 10**6, transcendentals=0),
        compiler_params=pltpu.CompilerParams(vmem_limit_bytes=24 << 20),
        name="select",
    )(ids, weights, in_hbm(cot))
    up = lax.ppermute(up, "pipe", [(i, i + 1) for i in range(pipe - 1)])
    got = lax.all_to_all(pay, "expert", 0, 0, tiled=True)
    u = gate_pre[0].reshape(2, slots, hidden)
    v = up_pre[0].reshape(2, slots, hidden)
    weights = [in_hbm(w[0]) for w in (w_down, w_gate, w_up)]
    piece = ((slots, width + 2 * hidden), BF16)
    ret, x0, x1, x2, x3 = call(
        expert_kernel,
        [((8 * n, width), BF16)] + [piece] * 4,
        2 * 10**9,
        8 * 10**6,
        (me, got.reshape(8 * n, width), u, v, *weights),
        held=weights,
        scratch_shapes=[pltpu.VMEM(w.shape, BF16) for w in weights] + [pltpu.SemaphoreType.DMA((3,))],
    )
    rows, meet = call(
        token_kernel, [((16, width), F32), ((16, 16), F32)], 10**9, 10**6, (up, sel0, in_hbm(cot)),
        held=[cot], scratch_shapes=[pltpu.VMEM(cot.shape, BF16), pltpu.SemaphoreType.DMA(())],
    )
    back = lax.all_to_all(ret.reshape(n, 8, width), "expert", 0, 0, tiled=True)
    (rows,) = call(combine_kernel, [((16, width), BF16)], 10**8, 10**6, (back, rows, meet))
    rows = lax.ppermute(rows, "pipe", [(i, i - 1) for i in range(1, pipe)])
    x1 = lax.ppermute(x1, "dp", [(i, i ^ 1) for i in range(N_DP)])
    x2 = lax.ppermute(x2, "dp", [(i, i ^ 2) for i in range(N_DP)])
    x3 = lax.ppermute(x3, "dp", [(i, i ^ 3) for i in range(N_DP)])
    rows = rows.reshape(EXP_FL, N_DP, 1, 2, width).swapaxes(0, 1)
    rows = jnp.broadcast_to(rows, (N_DP, EXP_FL, n // EXP_FL, 2, width))
    rows = rows.reshape(N_DP * n, 2, width)
    got = lax.all_to_all(rows, ("dp", "expert"), 0, 0, tiled=True)
    (acc,) = call(first_kernel, [((hidden, width), F32)], 10**8, 2 * 10**6, (x0, x1, x2, x3))
    (out,) = call(
        second_kernel,
        [((hidden, width), F32)],
        10**8,
        2 * 10**6,
        (me, acc, got.reshape(N_DP * slots, width), x0, x1, x2, x3),
        out_in_hbm=True,
    )
    return out[None]


def solution(mesh):
    in_specs = (
        P("pipe", ("dp", "expert"), None),
        P("pipe", None, ("dp", "expert"), None),
        P("pipe", None, ("dp", "expert"), None),
        P("pipe", None, "dp", None, None, "expert"),
        P("pipe", None, "dp", None, None, "expert"),
        P("pipe", None, "expert"),
        P("pipe", None, "expert"),
        P("pipe", "expert", None),
    )
    out_specs = P("pipe", "expert", "dp")

    return jax.shard_map(body, mesh=mesh, in_specs=in_specs, out_specs=out_specs, check_vma=False)
```
